32 devices in a mesh: group: 2 (over y), row: 4 (over z), col: 4 (over x, core).
Axes of the slice: x: 2, y: 2, z: 4, core: 2. Of those that a mesh axis runs over, the one named last changes fastest.
Arguments:
- compressed_absorbed_queries: bfloat16 [16, 128, 512], P(('group', 'row')), parts along dimension 0, may hold values from -6 to 6
- query_rope: bfloat16 [16, 64, 128], P(('group', 'row')), parts along dimension 0, may hold values from -6 to 6
- compressed_stored_keys: bfloat16 [16, 1024, 512], P(('group', 'row'), 'col'), parts along dimension 0, may hold values from -32 to 32
- cache_rope: bfloat16 [16, 64, 1024], P(('group', 'row'), None, 'col'), parts along dimension 0, may hold values from -32 to 32
- seq_lengths: int32 [16], P(('group', 'row')), parts along dimension 0, may hold values from 2 to 1024, as said below
- ffn_rows: bfloat16 [64, 7168], P(('group', 'row'), 'col'), parts along dimension 0, may hold values from -6 to 6
- norm_gain: bfloat16 [7168], P('col'), may hold values from 0.099609375 to 1.8984375
- w_gate: bfloat16 [7168, 18432], P('col', 'row'), may hold values from -0.0625 to 0.0625
- w_up: bfloat16 [7168, 18432], P('col', 'row'), may hold values from -0.0625 to 0.0625
- w_down: bfloat16 [18432, 7168], P('row', 'col'), may hold values from -0.046875 to 0.046875
Outputs:
- context: bfloat16 [16, 128, 512], P(('group', 'row'), 'col'), parts along dimension 0
- ffn_out: bfloat16 [64, 7168], P(('group', 'row'), 'col'), parts along dimension 0
The draws below stay inside these ranges and needn't reach their ends.
There are 2 independent parts, one for each index of `group`. The reference program is written for one: setup_inputs(seed, part) draws one part's arguments, and reference() takes and returns one part's arrays. A program takes and returns all parts, laid end to end along the dimension named above; an argument that names none is the same for every part. Nothing has to cross between parts.
Inputs may be any that keep to these rules, and one draw needn't show every extreme that they name: `seq_lengths`: each sequence has 2 to 1024 filled slots, the first ones of its cache, and some sequence has exactly 1024.
All inputs are finite; a program needn't handle non-finite values.
Results may differ from the reference program's by a relative error of at most 0.017.
Values may be sent and summed in bfloat16 or wider, within the bound.
A program may use at most 128 MiB of HBM per device.

```python
import jax
import jax.numpy as jnp
from jax import lax

D = 7168
FF = 18432
HEADS = 128
LATENT = 512
ROPE = 64
NOPE = 128
KV_LEN = 1024
SEQS = 8
TOKENS = 32


def length_law(key):
    counts = jax.random.randint(jax.random.fold_in(key, 301), (SEQS,), 2, KV_LEN + 1)
    chosen = jax.random.randint(jax.random.fold_in(key, 302), (), 0, SEQS)
    return jnp.where(jnp.arange(SEQS) == chosen, KV_LEN, counts).astype(jnp.int32)


def question_pieces(key):
    base = jax.random.fold_in(key, 101)
    shape = (SEQS, HEADS, LATENT + ROPE)
    full = jnp.clip(jax.random.normal(base, shape, jnp.float32), -6.0, 6.0)
    return full


def key_parts(key):
    width = LATENT + ROPE
    base = jax.random.fold_in(key, 202)
    full = jnp.clip(jax.random.normal(base, (SEQS, KV_LEN, width), jnp.float32), -6.0, 6.0)
    return full


def draw_compressed_absorbed_queries(key, part):
    return question_pieces(key)[:, :, :LATENT].astype(jnp.bfloat16)


def draw_query_rope(key, part):
    return jnp.transpose(question_pieces(key)[:, :, LATENT:], (0, 2, 1)).astype(jnp.bfloat16)


def draw_compressed_stored_keys(key, part):
    return key_parts(key)[:, :, :LATENT].astype(jnp.bfloat16)


def draw_cache_rope(key, part):
    return jnp.transpose(key_parts(key)[:, :, LATENT:], (0, 2, 1)).astype(jnp.bfloat16)


def draw_seq_lengths(key, part):
    return length_law(key)


def block_scale(stream_key, extent, pieces, smallest, largest):
    gain = 1.0
    for dim, shards_of in pieces:
        heights = jax.random.uniform(jax.random.fold_in(jax.random.fold_in(stream_key, 6), dim), (shards_of,), jnp.float32, smallest / len(pieces), largest / len(pieces))
        gain = gain * jnp.repeat(jnp.exp(heights), extent[dim] // shards_of).reshape((-1,) + (1,) * (len(extent) - 1 - dim))
    return gain


def centred(key, dims, scale, reach, split=(), held_as=jnp.bfloat16):
    values = jax.random.normal(key, dims, jnp.float32) * scale
    if len(split) > 0:
        values = block_scale(key, dims, split, -0.22, 0.18) * values
    return jnp.clip(values, min=-reach, max=reach).astype(held_as)


def setup_inputs(seed: int = 0, part: int = 0) -> dict:
    seeds = jax.random.split(jax.random.key(seed), 11)
    own_keys = jax.random.split(jax.random.fold_in(seeds[10], part), 11)
    compressed_absorbed_queries = draw_compressed_absorbed_queries(jax.random.fold_in(jax.random.fold_in(seeds[10], part), 71), part)
    query_rope = draw_query_rope(jax.random.fold_in(jax.random.fold_in(seeds[10], part), 71), part)
    compressed_stored_keys = draw_compressed_stored_keys(jax.random.fold_in(jax.random.fold_in(seeds[10], part), 71), part)
    cache_rope = draw_cache_rope(jax.random.fold_in(jax.random.fold_in(seeds[10], part), 71), part)
    seq_lengths = draw_seq_lengths(jax.random.fold_in(jax.random.fold_in(seeds[10], part), 71), part)
    ffn_rows = centred(own_keys[5], (TOKENS, D), 1.0, 6.0, ((0, 4), (1, 4)))
    norm_gain = jnp.clip(1.0 + 0.18 * jax.random.normal(seeds[6], (D,), jnp.float32), 0.099609375, 1.8984375).astype(jnp.bfloat16)
    w_gate = centred(seeds[7], (D, FF), D ** -0.5, 0.0625, ((0, 4), (1, 4)))
    w_up = centred(seeds[8], (D, FF), D ** -0.5, 0.0625, ((0, 4), (1, 4)))
    w_down = centred(seeds[9], (FF, D), FF ** -0.5, 0.046875, ((0, 4), (1, 4)))
    return dict(compressed_absorbed_queries=compressed_absorbed_queries, query_rope=query_rope, compressed_stored_keys=compressed_stored_keys, cache_rope=cache_rope, seq_lengths=seq_lengths, ffn_rows=ffn_rows, norm_gain=norm_gain, w_gate=w_gate, w_up=w_up, w_down=w_down)


NEGATIVE_PADDING = -1e+30

def attend_one(packed):
    latent_query, rotary_query_part, latent_keys, rope_keys, length_one = packed
    similarity_logits = jnp.dot(latent_query, latent_keys.T, preferred_element_type=jnp.float32)
    similarity_logits = similarity_logits + jnp.dot(rotary_query_part.T, rope_keys, preferred_element_type=jnp.float32)
    similarity_logits = similarity_logits * (NOPE + ROPE) ** (-0.5)
    position = jnp.arange(KV_LEN, dtype=jnp.int32)
    visible = (position < length_one)[None, :]
    similarity_logits = jnp.where(visible, similarity_logits, NEGATIVE_PADDING)
    top_score = lax.optimization_barrier(jnp.max(similarity_logits, axis=1, keepdims=True))
    weights = jnp.where(visible, jnp.exp(similarity_logits - top_score), 0.0)
    denominator = lax.optimization_barrier(jnp.sum(weights, axis=1, keepdims=True))
    weighted = jnp.dot(weights.astype(jnp.bfloat16), latent_keys, preferred_element_type=jnp.float32)
    return (weighted / denominator).astype(jnp.bfloat16)

def reference(compressed_absorbed_queries, query_rope, compressed_stored_keys, cache_rope, seq_lengths, ffn_rows, norm_gain, w_gate, w_up, w_down):
    context = lax.map(attend_one, (compressed_absorbed_queries, query_rope, compressed_stored_keys, cache_rope, seq_lengths))
    rows_wide = ffn_rows.astype(jnp.float32)
    mean_square = lax.optimization_barrier(jnp.mean(rows_wide * rows_wide, axis=1, keepdims=True))
    normed = (rows_wide * lax.rsqrt(mean_square + 1e-06) * norm_gain.astype(jnp.float32)).astype(jnp.bfloat16)
    gate = jnp.dot(normed, w_gate, preferred_element_type=jnp.float32)
    up_proj = jnp.dot(normed, w_up, preferred_element_type=jnp.float32)
    hidden = (jax.nn.silu(gate) * up_proj).astype(jnp.bfloat16)
    ffn_out = (rows_wide + jnp.dot(hidden, w_down, preferred_element_type=jnp.float32)).astype(jnp.bfloat16)
    return (context, ffn_out)
```

```python
import functools

import jax
import jax.numpy as jnp
from jax import lax
from jax.experimental import pallas as pl
from jax.experimental.pallas import tpu as pltpu
from jax.sharding import PartitionSpec as P

NOPE = 128
NEGATIVE_PADDING = -1e30
F32 = jnp.float32
BF16 = jnp.bfloat16


def kernel(
    nrow, ncol, chunks,
    q_hbm, qr_hbm, k_hbm, kr_hbm, lens, x_hbm, gain_hbm, wg_hbm, wu_hbm, wd_hbm,
    ctx_ref, out_ref,
    q, qr, k, kr, gain, xall, xg, wg, wu, wd,
    att, stat, att_in, stat_in, sq, sq_in,
    gu, gu_in, hid, acc, dn, dn_in,
    in_sem, w_sem, x_ss, x_rs, att_ss, att_rs, stat_ss, stat_rs, sq_ss, sq_rs,
    gu_ss, gu_rs, h_ss, h_rs, dn_ss, dn_rs,
):
    r = lax.axis_index("row")
    c = lax.axis_index("col")
    seqs, heads, latent = q_hbm.shape
    rope = qr_hbm.shape[1]
    slots = k_hbm.shape[1]
    own_rows, feats = x_hbm.shape
    units = wg_hbm.shape[1]
    nb = units // chunks
    tokens = own_rows * nrow
    tb = tokens // ncol
    hs = heads // ncol

    small = [
        pltpu.make_async_copy(x_hbm, xall.at[r], in_sem.at[0]),
        pltpu.make_async_copy(gain_hbm, gain, in_sem.at[1]),
        pltpu.make_async_copy(q_hbm, q, in_sem.at[2]),
        pltpu.make_async_copy(qr_hbm, qr, in_sem.at[3]),
        pltpu.make_async_copy(k_hbm, k, in_sem.at[4]),
        pltpu.make_async_copy(kr_hbm, kr, in_sem.at[5]),
    ]
    for copy in small:
        copy.start()

    def weight_copies(j):
        if chunks == 1:
            return (
                pltpu.make_async_copy(wg_hbm, wg.at[0], w_sem.at[0, 0]),
                pltpu.make_async_copy(wu_hbm, wu.at[0], w_sem.at[1, 0]),
                pltpu.make_async_copy(wd_hbm, wd.at[0], w_sem.at[2, 0]),
            )
        cut = pl.ds(pl.multiple_of(j * nb, 128), nb)
        return (
            pltpu.make_async_copy(wg_hbm.at[:, cut], wg.at[j], w_sem.at[0, j]),
            pltpu.make_async_copy(wu_hbm.at[:, cut], wu.at[j], w_sem.at[1, j]),
            pltpu.make_async_copy(wd_hbm.at[cut, :], wd.at[j], w_sem.at[2, j]),
        )

    for j in range(chunks):
        copies = weight_copies(j)
        copies[0].start()
        copies[1].start()
    for j in range(chunks):
        weight_copies(j)[2].start()

    barrier = pltpu.get_barrier_semaphore()
    for d in range(1, nrow):
        pl.semaphore_signal(barrier, inc=1, device_id={"row": lax.rem(r + d, nrow)},
                            device_id_type=pl.DeviceIdType.MESH)
    for d in range(1, ncol):
        pl.semaphore_signal(barrier, inc=1, device_id={"col": lax.rem(c + d, ncol)},
                            device_id_type=pl.DeviceIdType.MESH)
    pl.semaphore_wait(barrier, nrow + ncol - 2)

    def remote(src, dst, send, recv, axis, peer):
        return pltpu.make_async_remote_copy(
            src_ref=src, dst_ref=dst, send_sem=send, recv_sem=recv,
            device_id={axis: peer}, device_id_type=pl.DeviceIdType.MESH)

    def x_copy(d, source):
        return remote(xall.at[r], xall.at[source], x_ss.at[d - 1], x_rs.at[d - 1],
                      "row", lax.rem(r + d, nrow))

    small[0].wait()
    for d in range(1, nrow):
        x_copy(d, r).start()

    def att_copies(d):
        peer = lax.rem(c + d, ncol)
        return (
            remote(att.at[peer], att_in.at[d - 1], att_ss.at[d - 1], att_rs.at[d - 1], "col", peer),
            remote(stat.at[peer], stat_in.at[d - 1], stat_ss.at[d - 1], stat_rs.at[d - 1], "col", peer),
        )

    for copy in small[1:]:
        copy.wait()
    position = c * slots + lax.broadcasted_iota(jnp.int32, (1, slots), 1)
    lane = lax.broadcasted_iota(jnp.int32, (1, 128), 1)
    for s in range(seqs):
        keys = k[s]
        logits = lax.dot_general(q[s], keys, (((1,), (1,)), ((), ())), preferred_element_type=F32)
        logits = logits + lax.dot_general(
            qr[s], kr[s], (((0,), (0,)), ((), ())), preferred_element_type=F32)
        logits = logits * (NOPE + rope) ** (-0.5)
        visible = position < lens[s]
        logits = jnp.where(visible, logits, NEGATIVE_PADDING)
        top = jnp.max(logits, axis=1, keepdims=True)
        weights = jnp.where(visible, jnp.exp(logits - top), 0.0)
        total = jnp.sum(weights, axis=1, keepdims=True)
        weighted = jnp.dot(weights.astype(BF16), keys, preferred_element_type=F32)
        both = jnp.where(lane < 64, top, total)
        for p in range(ncol):
            cut = slice(p * hs, (p + 1) * hs)
            att[p, s] = weighted[cut].astype(BF16)
            stat[p, s] = both[cut]
    for d in range(1, ncol):
        for copy in att_copies(d):
            copy.start()

    for d in range(1, nrow):
        x_copy(d, lax.rem(r - d + nrow, nrow)).wait()
    wide = xall[...].astype(F32).reshape(tokens, feats)
    squares = jnp.sum(wide * wide, axis=1, keepdims=True)
    sq[...] = jnp.broadcast_to(squares, (tokens, 128)).reshape(ncol, tb, 128)
    xg[...] = (wide * gain[...].astype(F32)).astype(BF16)

    def sq_copy(d):
        peer = lax.rem(c + d, ncol)
        return remote(sq.at[peer], sq_in.at[d - 1], sq_ss.at[d - 1], sq_rs.at[d - 1], "col", peer)

    for d in range(1, ncol):
        sq_copy(d).start()

    def gu_copy(j, d):
        peer = lax.rem(c + d, ncol)
        return remote(gu.at[j, peer], gu_in.at[j, d - 1], gu_ss.at[j, d - 1], gu_rs.at[j, d - 1],
                      "col", peer)

    def h_copy(j, d, source):
        return remote(hid.at[j, c], hid.at[j, source], h_ss.at[j, d - 1], h_rs.at[j, d - 1],
                      "col", lax.rem(c + d, ncol))

    def project(j):
        copies = weight_copies(j)
        copies[0].wait()
        gate = jnp.dot(xg[...], wg[j], preferred_element_type=F32).astype(BF16)
        for p in range(ncol):
            gu[j, p, 0] = gate[p * tb:(p + 1) * tb]
        copies[1].wait()
        up = jnp.dot(xg[...], wu[j], preferred_element_type=F32).astype(BF16)
        for p in range(ncol):
            gu[j, p, 1] = up[p * tb:(p + 1) * tb]
        for d in range(1, ncol):
            gu_copy(j, d).start()

    def activate(j, norm):
        for d in range(1, ncol):
            gu_copy(j, d).wait_recv()
        gate = gu[j, c, 0].astype(F32)
        up = gu[j, c, 1].astype(F32)
        for d in range(1, ncol):
            gate = gate + gu_in[j, d - 1, 0].astype(F32)
            up = up + gu_in[j, d - 1, 1].astype(F32)
        gate = gate * norm
        hid[j, c] = (gate / (1.0 + jnp.exp(-gate)) * (up * norm)).astype(BF16)
        for d in range(1, ncol):
            h_copy(j, d, c).start()

    project(0)
    for d in range(1, ncol):
        sq_copy(d).wait()
    mean = sq[c]
    for d in range(1, ncol):
        mean = mean + sq_in[d - 1]
    norm = lax.rsqrt(mean[:, :1] / (feats * ncol) + 1e-06)

    @pl.loop(1, chunks)
    def _(j):
        project(j)
        activate(j - 1, norm)

    activate(chunks - 1, norm)

    acc[...] = jnp.zeros_like(acc)

    @pl.loop(0, chunks)
    def _(j):
        weight_copies(j)[2].wait()
        for d in range(1, ncol):
            h_copy(j, d, lax.rem(c - d + ncol, ncol)).wait_recv()
        hidden = hid[j].astype(F32).reshape(tokens, nb).astype(BF16)
        acc[...] += jnp.dot(hidden, wd[j], preferred_element_type=F32)

    dn[...] = acc[...].reshape(nrow, own_rows, feats).astype(BF16)

    def dn_copy(d):
        peer = lax.rem(r + d, nrow)
        return remote(dn.at[peer], dn_in.at[d - 1], dn_ss.at[d - 1], dn_rs.at[d - 1], "row", peer)

    for d in range(1, nrow):
        dn_copy(d).start()

    for d in range(1, ncol):
        for copy in att_copies(d):
            copy.wait()
    for s in range(seqs):
        tops = [stat[c, s, :, 0:1]] + [stat_in[d - 1, s, :, 0:1] for d in range(1, ncol)]
        totals = [stat[c, s, :, 64:65]] + [stat_in[d - 1, s, :, 64:65] for d in range(1, ncol)]
        parts = [att[c, s]] + [att_in[d - 1, s] for d in range(1, ncol)]
        top = functools.reduce(jnp.maximum, tops)
        factors = [jnp.exp(t - top) for t in tops]
        total = sum(f * t for f, t in zip(factors, totals))
        weighted = sum(f * w.astype(F32) for f, w in zip(factors, parts))
        ctx_ref[s] = (weighted / total).astype(BF16)

    own = xall[r].astype(F32)
    summed = acc[pl.ds(pl.multiple_of(r * own_rows, own_rows), own_rows), :]
    for d in range(1, nrow):
        dn_copy(d).wait()
        summed = summed + dn_in[d - 1].astype(F32)
    out_ref[...] = (own + summed).astype(BF16)

    @pl.loop(0, chunks)
    def _(j):
        for d in range(1, ncol):
            gu_copy(j, d).wait_send()
            h_copy(j, d, c).wait_send()


def on_device(nrow, ncol, q, qr, k, kr, lens, x, gain, wg, wu, wd):
    seqs, heads, latent = q.shape
    own_rows, feats = x.shape
    units = wg.shape[1]
    tokens = own_rows * nrow
    tb, hs = tokens // ncol, heads // ncol
    chunks = 1
    for n in (6, 4, 3, 2):
        if units % (256 * n) == 0:
            chunks = n
            break
    nb = units // chunks
    dma = pltpu.SemaphoreType.DMA
    anywhere = pl.BlockSpec(memory_space=pl.ANY)
    vmem = pl.BlockSpec(memory_space=pltpu.VMEM)
    return pl.pallas_call(
        functools.partial(kernel, nrow, ncol, chunks),
        out_shape=(
            jax.ShapeDtypeStruct((seqs, hs, latent), BF16),
            jax.ShapeDtypeStruct((own_rows, feats), BF16),
        ),
        in_specs=[anywhere] * 4 + [pl.BlockSpec(memory_space=pltpu.SMEM)] + [anywhere] * 5,
        out_specs=(vmem, vmem),
        scratch_shapes=[
            pltpu.VMEM(q.shape, BF16),
            pltpu.VMEM(qr.shape, BF16),
            pltpu.VMEM(k.shape, BF16),
            pltpu.VMEM(kr.shape, BF16),
            pltpu.VMEM((1, feats), BF16),
            pltpu.VMEM((nrow, own_rows, feats), BF16),
            pltpu.VMEM((tokens, feats), BF16),
            pltpu.VMEM((chunks, feats, nb), BF16),
            pltpu.VMEM((chunks, feats, nb), BF16),
            pltpu.VMEM((chunks, nb, feats), BF16),
            pltpu.VMEM((ncol, seqs, hs, latent), BF16),
            pltpu.VMEM((ncol, seqs, hs, 128), F32),
            pltpu.VMEM((ncol - 1, seqs, hs, latent), BF16),
            pltpu.VMEM((ncol - 1, seqs, hs, 128), F32),
            pltpu.VMEM((ncol, tb, 128), F32),
            pltpu.VMEM((ncol - 1, tb, 128), F32),
            pltpu.VMEM((chunks, ncol, 2, tb, nb), BF16),
            pltpu.VMEM((chunks, ncol - 1, 2, tb, nb), BF16),
            pltpu.VMEM((chunks, ncol, tb, nb), BF16),
            pltpu.VMEM((tokens, feats), F32),
            pltpu.VMEM((nrow, own_rows, feats), BF16),
            pltpu.VMEM((nrow - 1, own_rows, feats), BF16),
            dma((6,)),
            dma((3, chunks)),
            dma((nrow - 1,)), dma((nrow - 1,)),
            dma((ncol - 1,)), dma((ncol - 1,)),
            dma((ncol - 1,)), dma((ncol - 1,)),
            dma((ncol - 1,)), dma((ncol - 1,)),
            dma((chunks, ncol - 1)), dma((chunks, ncol - 1)),
            dma((chunks, ncol - 1)), dma((chunks, ncol - 1)),
            dma((nrow - 1,)), dma((nrow - 1,)),
        ],
        compiler_params=pltpu.CompilerParams(
            collective_id=0, has_side_effects=True, vmem_limit_bytes=67043328
        ),
    )(q, qr, k, kr, lens, x, gain[None, :], wg, wu, wd)


def solution(mesh):
    return jax.shard_map(
        functools.partial(on_device, mesh.shape["row"], mesh.shape["col"]),
        mesh=mesh,
        in_specs=(
            P(("group", "row"), None, None),
            P(("group", "row"), None, None),
            P(("group", "row"), "col", None),
            P(("group", "row"), None, "col"),
            P(("group", "row")),
            P(("group", "row"), "col"),
            P("col"),
            P("col", "row"),
            P("col", "row"),
            P("row", "col"),
        ),
        out_specs=(P(("group", "row"), "col", None), P(("group", "row"), "col")),
        check_vma=False,
    )
```

```python
import functools

import jax
import jax.numpy as jnp
from jax import lax
from jax.experimental import pallas as pl
from jax.experimental.pallas import tpu as pltpu
from jax.sharding import PartitionSpec as P

NOPE = 128
NEGATIVE_PADDING = -1e30
F32 = jnp.float32
BF16 = jnp.bfloat16


def kernel(
    nrow, ncol, chunks,
    q_hbm, qr_hbm, k_hbm, kr_hbm, lens, x_hbm, gain_hbm, wg_hbm, wu_hbm, wd_hbm,
    ctx_ref, out_ref,
    q, qr, k, kr, gain, xall, xg, wg, wu, wd,
    att, stat, att_in, stat_in, sq, sq_in,
    gu, gu_in, hid, acc, dn, dn_in,
    in_sem, w_sem, x_ss, x_rs, att_ss, att_rs, stat_ss, stat_rs, sq_ss, sq_rs,
    gu_ss, gu_rs, h_ss, h_rs, dn_ss, dn_rs,
):
    r = lax.axis_index("row")
    c = lax.axis_index("col")
    seqs, heads, latent = q_hbm.shape
    rope = qr_hbm.shape[1]
    slots = k_hbm.shape[1]
    own_rows, feats = x_hbm.shape
    units = wg_hbm.shape[1]
    nb = units // chunks
    tokens = own_rows * nrow
    tb = tokens // ncol
    hs = heads // ncol

    small = [
        pltpu.make_async_copy(x_hbm, xall.at[r], in_sem.at[0]),
        pltpu.make_async_copy(gain_hbm, gain, in_sem.at[1]),
        pltpu.make_async_copy(q_hbm, q, in_sem.at[2]),
        pltpu.make_async_copy(qr_hbm, qr, in_sem.at[3]),
        pltpu.make_async_copy(k_hbm, k, in_sem.at[4]),
        pltpu.make_async_copy(kr_hbm, kr, in_sem.at[5]),
    ]
    for copy in small:
        copy.start()

    def weight_copies(j):
        if chunks == 1:
            return (
                pltpu.make_async_copy(wg_hbm, wg.at[0], w_sem.at[0, 0]),
                pltpu.make_async_copy(wu_hbm, wu.at[0], w_sem.at[1, 0]),
                pltpu.make_async_copy(wd_hbm, wd.at[0], w_sem.at[2, 0]),
            )
        cut = pl.ds(pl.multiple_of(j * nb, 128), nb)
        return (
            pltpu.make_async_copy(wg_hbm.at[:, cut], wg.at[j], w_sem.at[0, j]),
            pltpu.make_async_copy(wu_hbm.at[:, cut], wu.at[j], w_sem.at[1, j]),
            pltpu.make_async_copy(wd_hbm.at[cut, :], wd.at[j], w_sem.at[2, j]),
        )

    for j in range(chunks):
        copies = weight_copies(j)
        copies[0].start()
        copies[1].start()
    for j in range(chunks):
        weight_copies(j)[2].start()

    barrier = pltpu.get_barrier_semaphore()
    for d in range(1, nrow):
        pl.semaphore_signal(barrier, inc=1, device_id={"row": lax.rem(r + d, nrow)},
                            device_id_type=pl.DeviceIdType.MESH)
    for d in range(1, ncol):
        pl.semaphore_signal(barrier, inc=1, device_id={"col": lax.rem(c + d, ncol)},
                            device_id_type=pl.DeviceIdType.MESH)
    pl.semaphore_wait(barrier, nrow + ncol - 2)

    def remote(src, dst, send, recv, axis, peer):
        return pltpu.make_async_remote_copy(
            src_ref=src, dst_ref=dst, send_sem=send, recv_sem=recv,
            device_id={axis: peer}, device_id_type=pl.DeviceIdType.MESH)

    def x_copy(d, source):
        return remote(xall.at[r], xall.at[source], x_ss.at[d - 1], x_rs.at[d - 1],
                      "row", lax.rem(r + d, nrow))

    small[0].wait()
    for d in range(1, nrow):
        x_copy(d, r).start()

    def att_copies(d):
        peer = lax.rem(c + d, ncol)
        return (
            remote(att.at[peer], att_in.at[d - 1], att_ss.at[d - 1], att_rs.at[d - 1], "col", peer),
            remote(stat.at[peer], stat_in.at[d - 1], stat_ss.at[d - 1], stat_rs.at[d - 1], "col", peer),
        )

    for copy in small[1:]:
        copy.wait()
    position = c * slots + lax.broadcasted_iota(jnp.int32, (1, slots), 1)
    lane = lax.broadcasted_iota(jnp.int32, (1, 128), 1)
    for s in range(seqs):
        keys = k[s]
        logits = lax.dot_general(q[s], keys, (((1,), (1,)), ((), ())), preferred_element_type=F32)
        logits = logits + lax.dot_general(
            qr[s], kr[s], (((0,), (0,)), ((), ())), preferred_element_type=F32)
        logits = logits * (NOPE + rope) ** (-0.5)
        visible = position < lens[s]
        logits = jnp.where(visible, logits, NEGATIVE_PADDING)
        top = jnp.max(logits, axis=1, keepdims=True)
        weights = jnp.where(visible, jnp.exp(logits - top), 0.0)
        total = jnp.sum(weights, axis=1, keepdims=True)
        weighted = jnp.dot(weights.astype(BF16), keys, preferred_element_type=F32)
        both = jnp.where(lane < 64, top, total)
        for p in range(ncol):
            cut = slice(p * hs, (p + 1) * hs)
            att[p, s] = weighted[cut].astype(BF16)
            stat[p, s] = both[cut]
    for d in range(1, ncol):
        for copy in att_copies(d):
            copy.start()

    for d in range(1, nrow):
        x_copy(d, lax.rem(r - d + nrow, nrow)).wait()
    wide = xall[...].astype(F32).reshape(tokens, feats)
    squares = jnp.sum(wide * wide, axis=1, keepdims=True)
    sq[...] = jnp.broadcast_to(squares, (tokens, 128)).reshape(ncol, tb, 128)
    xg[...] = (wide * gain[...].astype(F32)[None, :]).astype(BF16)

    def sq_copy(d):
        peer = lax.rem(c + d, ncol)
        return remote(sq.at[peer], sq_in.at[d - 1], sq_ss.at[d - 1], sq_rs.at[d - 1], "col", peer)

    for d in range(1, ncol):
        sq_copy(d).start()

    def gu_copy(j, d):
        peer = lax.rem(c + d, ncol)
        return remote(gu.at[j, peer], gu_in.at[j, d - 1], gu_ss.at[j, d - 1], gu_rs.at[j, d - 1],
                      "col", peer)

    def h_copy(j, d, source):
        return remote(hid.at[j, c], hid.at[j, source], h_ss.at[j, d - 1], h_rs.at[j, d - 1],
                      "col", lax.rem(c + d, ncol))

    def project(j):
        copies = weight_copies(j)
        copies[0].wait()
        gate = jnp.dot(xg[...], wg[j], preferred_element_type=F32).astype(BF16)
        for p in range(ncol):
            gu[j, p, 0] = gate[p * tb:(p + 1) * tb]
        copies[1].wait()
        up = jnp.dot(xg[...], wu[j], preferred_element_type=F32).astype(BF16)
        for p in range(ncol):
            gu[j, p, 1] = up[p * tb:(p + 1) * tb]
        for d in range(1, ncol):
            gu_copy(j, d).start()

    def activate(j, norm):
        for d in range(1, ncol):
            gu_copy(j, d).wait_recv()
        gate = gu[j, c, 0].astype(F32)
        up = gu[j, c, 1].astype(F32)
        for d in range(1, ncol):
            gate = gate + gu_in[j, d - 1, 0].astype(F32)
            up = up + gu_in[j, d - 1, 1].astype(F32)
        gate = gate * norm
        hid[j, c] = (gate / (1.0 + jnp.exp(-gate)) * (up * norm)).astype(BF16)
        for d in range(1, ncol):
            h_copy(j, d, c).start()

    project(0)
    for d in range(1, ncol):
        sq_copy(d).wait()
    mean = sq[c]
    for d in range(1, ncol):
        mean = mean + sq_in[d - 1]
    norm = lax.rsqrt(mean[:, :1] / (feats * ncol) + 1e-06)

    lag = min(3, chunks)

    @pl.loop(1, lag)
    def _(j):
        project(j)

    @pl.loop(lag, chunks)
    def _(j):
        project(j)
        activate(j - lag, norm)

    @pl.loop(chunks - lag, chunks)
    def _(j):
        activate(j, norm)

    acc[...] = jnp.zeros_like(acc)

    @pl.loop(0, chunks)
    def _(j):
        weight_copies(j)[2].wait()
        for d in range(1, ncol):
            h_copy(j, d, lax.rem(c - d + ncol, ncol)).wait_recv()
        hidden = hid[j].astype(F32).reshape(tokens, nb).astype(BF16)
        acc[...] += jnp.dot(hidden, wd[j], preferred_element_type=F32)

    dn[...] = acc[...].reshape(nrow, own_rows, feats).astype(BF16)

    def dn_copy(d):
        peer = lax.rem(r + d, nrow)
        return remote(dn.at[peer], dn_in.at[d - 1], dn_ss.at[d - 1], dn_rs.at[d - 1], "row", peer)

    for d in range(1, nrow):
        dn_copy(d).start()

    for d in range(1, ncol):
        for copy in att_copies(d):
            copy.wait()
    for s in range(seqs):
        tops = [stat[c, s, :, 0:1]] + [stat_in[d - 1, s, :, 0:1] for d in range(1, ncol)]
        totals = [stat[c, s, :, 64:65]] + [stat_in[d - 1, s, :, 64:65] for d in range(1, ncol)]
        parts = [att[c, s]] + [att_in[d - 1, s] for d in range(1, ncol)]
        top = functools.reduce(jnp.maximum, tops)
        factors = [jnp.exp(t - top) for t in tops]
        total = sum(f * t for f, t in zip(factors, totals))
        weighted = sum(f * w.astype(F32) for f, w in zip(factors, parts))
        ctx_ref[s] = (weighted / total).astype(BF16)

    own = xall[r].astype(F32)
    summed = acc[pl.ds(pl.multiple_of(r * own_rows, own_rows), own_rows), :]
    for d in range(1, nrow):
        dn_copy(d).wait()
        summed = summed + dn_in[d - 1].astype(F32)
    out_ref[...] = (own + summed).astype(BF16)

    @pl.loop(0, chunks)
    def _(j):
        for d in range(1, ncol):
            gu_copy(j, d).wait_send()
            h_copy(j, d, c).wait_send()


def on_device(nrow, ncol, q, qr, k, kr, lens, x, gain, wg, wu, wd):
    seqs, heads, latent = q.shape
    own_rows, feats = x.shape
    units = wg.shape[1]
    tokens = own_rows * nrow
    tb, hs = tokens // ncol, heads // ncol
    chunks = 1
    for n in (3, 4, 6, 2):
        if units % (256 * n) == 0:
            chunks = n
            break
    nb = units // chunks
    dma = pltpu.SemaphoreType.DMA
    anywhere = pl.BlockSpec(memory_space=pl.ANY)
    vmem = pl.BlockSpec(memory_space=pltpu.VMEM)
    return pl.pallas_call(
        functools.partial(kernel, nrow, ncol, chunks),
        out_shape=(
            jax.ShapeDtypeStruct((seqs, hs, latent), BF16),
            jax.ShapeDtypeStruct((own_rows, feats), BF16),
        ),
        in_specs=[anywhere] * 4 + [pl.BlockSpec(memory_space=pltpu.SMEM)] + [anywhere] * 5,
        out_specs=(vmem, vmem),
        scratch_shapes=[
            pltpu.VMEM(q.shape, BF16),
            pltpu.VMEM(qr.shape, BF16),
            pltpu.VMEM(k.shape, BF16),
            pltpu.VMEM(kr.shape, BF16),
            pltpu.VMEM((feats,), BF16),
            pltpu.VMEM((nrow, own_rows, feats), BF16),
            pltpu.VMEM((tokens, feats), BF16),
            pltpu.VMEM((chunks, feats, nb), BF16),
            pltpu.VMEM((chunks, feats, nb), BF16),
            pltpu.VMEM((chunks, nb, feats), BF16),
            pltpu.VMEM((ncol, seqs, hs, latent), BF16),
            pltpu.VMEM((ncol, seqs, hs, 128), F32),
            pltpu.VMEM((ncol - 1, seqs, hs, latent), BF16),
            pltpu.VMEM((ncol - 1, seqs, hs, 128), F32),
            pltpu.VMEM((ncol, tb, 128), F32),
            pltpu.VMEM((ncol - 1, tb, 128), F32),
            pltpu.VMEM((chunks, ncol, 2, tb, nb), BF16),
            pltpu.VMEM((chunks, ncol - 1, 2, tb, nb), BF16),
            pltpu.VMEM((chunks, ncol, tb, nb), BF16),
            pltpu.VMEM((tokens, feats), F32),
            pltpu.VMEM((nrow, own_rows, feats), BF16),
            pltpu.VMEM((nrow - 1, own_rows, feats), BF16),
            dma((6,)),
            dma((3, chunks)),
            dma((nrow - 1,)), dma((nrow - 1,)),
            dma((ncol - 1,)), dma((ncol - 1,)),
            dma((ncol - 1,)), dma((ncol - 1,)),
            dma((ncol - 1,)), dma((ncol - 1,)),
            dma((chunks, ncol - 1)), dma((chunks, ncol - 1)),
            dma((chunks, ncol - 1)), dma((chunks, ncol - 1)),
            dma((nrow - 1,)), dma((nrow - 1,)),
        ],
        compiler_params=pltpu.CompilerParams(
            collective_id=0, has_side_effects=True, vmem_limit_bytes=67043328
        ),
    )(q, qr, k, kr, lens, x, gain, wg, wu, wd)


def solution(mesh):
    return jax.shard_map(
        functools.partial(on_device, mesh.shape["row"], mesh.shape["col"]),
        mesh=mesh,
        in_specs=(
            P(("group", "row"), None, None),
            P(("group", "row"), None, None),
            P(("group", "row"), "col", None),
            P(("group", "row"), None, "col"),
            P(("group", "row")),
            P(("group", "row"), "col"),
            P("col"),
            P("col", "row"),
            P("col", "row"),
            P("row", "col"),
        ),
        out_specs=(P(("group", "row"), "col", None), P(("group", "row"), "col")),
        check_vma=False,
    )
```
